32 devices in a mesh: clus: 4 (over z), seq: 8 (over y, x, core).
Axes of the slice: x: 2, y: 2, z: 4, core: 2. Of those that a mesh axis runs over, the one named last changes fastest.
Arguments:
- embeddings: bfloat16 [8192, 768], P(('clus', 'seq')), parts along dimension 0, may hold values from -1 to 1, as said below
- doc_order: int32 [32, 256], P(('clus', 'seq')), parts along dimension 0, may hold values from 0 to 255, each once within a row
Outputs:
- prior_max: float32 [8192], P(('clus', 'seq')), parts along dimension 0
- later_max: float32 [8192], P(('clus', 'seq')), parts along dimension 0
The draws below stay inside these ranges and needn't reach their ends.
There are 4 independent parts, one for each index of `clus`. The reference program is written for one: setup_inputs(seed, part) draws one part's arguments, and reference() takes and returns one part's arrays. A program takes and returns all parts, laid end to end along the dimension named above; each array names one. Nothing has to cross between parts.
Inputs may be any that keep to these rules, and one draw needn't show every extreme that they name: `embeddings`: each row has unit Euclidean length up to bfloat16 rounding. `doc_order`: each row is a permutation of 0 to 255.
All inputs are finite; a program needn't handle non-finite values.
Results may differ from the reference program's by a relative error of at most 0.0003.
Values may be sent and summed in bfloat16 or wider, within the bound.
A program may use at most 64 MiB of HBM per device.

```python
import jax
import jax.numpy as jnp
from jax import lax

D = 768
BLK = 256
BLOCKS = 8
ROWS = 2048


def draw_embeddings(key, part):
    key_noise = jax.random.fold_in(key, 11)
    key_center = jax.random.fold_in(key, 12)
    key_weight = jax.random.fold_in(key, 13)
    key_assign = jax.random.fold_in(key, 14)
    center_count = 32
    assign = jax.random.randint(key_assign, (ROWS,), 0, center_count)
    centers = jax.random.normal(key_center, (center_count, D), jnp.float32)
    noise = jax.random.normal(key_noise, (ROWS, D), jnp.float32)
    weight = jax.random.uniform(key_weight, (ROWS,), jnp.float32, 0.6, 1.6)
    chosen = centers[assign]
    mixed = noise + weight[:, None] * chosen
    length = jnp.sqrt(jnp.sum(mixed * mixed, axis=1, keepdims=True))
    return (mixed / length).astype(jnp.bfloat16)


def setup_inputs(seed: int = 0, part: int = 0) -> dict:
    keys = jax.random.split(jax.random.key(seed), 3)
    own_keys = jax.random.split(jax.random.fold_in(keys[2], part), 3)
    embeddings = draw_embeddings(jax.random.fold_in(jax.random.fold_in(keys[2], part), 71), part)
    doc_order = jax.vmap(lambda own: jax.random.permutation(own, BLK))(jax.random.split(own_keys[1], BLOCKS)).reshape((BLOCKS, BLK)).astype(jnp.int32)
    return dict(embeddings=embeddings, doc_order=doc_order)


def reference(embeddings, doc_order):
    members = embeddings.astype(jnp.float32)
    ranking = doc_order.reshape(ROWS)
    column_block = (jnp.arange(ROWS, dtype=jnp.int32) // BLK).astype(jnp.int32)

    def one_block(block_index):
        rows_here = lax.dynamic_slice_in_dim(members, (block_index * BLK).astype(jnp.int32), BLK, 0)
        rank_here = lax.dynamic_slice_in_dim(ranking, (block_index * BLK).astype(jnp.int32), BLK, 0)
        similar = jnp.dot(rows_here, members.T, precision=lax.Precision.HIGHEST, preferred_element_type=jnp.float32)
        same_block = (column_block == block_index)[None, :]
        before = (column_block < block_index)[None, :] | (same_block & (ranking[None, :] < rank_here[:, None]))
        after = (column_block > block_index)[None, :] | (same_block & (ranking[None, :] > rank_here[:, None]))
        prior_part = jnp.max(jnp.where(before, similar, jnp.float32(-1.0)), axis=1)
        later_part = jnp.max(jnp.where(after, similar, jnp.float32(-1.0)), axis=1)
        return prior_part, later_part

    prior_parts, later_parts = lax.map(one_block, jnp.arange(BLOCKS, dtype=jnp.int32))
    return prior_parts.reshape(ROWS), later_parts.reshape(ROWS)
```

```python
import functools

import jax
import jax.numpy as jnp
from jax import lax
from jax.experimental import pallas as pl
from jax.experimental.pallas import tpu as pltpu
from jax.sharding import PartitionSpec as P

MESH = pl.DeviceIdType.MESH
PIECES = 2


def column_max(left, right):
    sims = lax.dot_general(
        left, right, (((1,), (1,)), ((), ())), preferred_element_type=jnp.float32
    )
    return jnp.max(sims, axis=0, keepdims=True)


def exchange_kernel(
    emb_hbm, rank_ref, prior_ref, later_ref,
    own, mate, xblk, yblk, mate_out, x_out, y_out, mate_in, x_in, y_in,
    load_sem, mate_sems, x_send, x_recv, y_send, y_recv, back_send, back_recv,
):
    me = lax.axis_index("seq")
    core, xbit, ybit = me % 2, (me // 2) % 2, me // 4
    rows = own.shape[0]
    piece = rows // PIECES
    mate_id = me + 1 - 2 * core
    x_id = me + 2 - 4 * xbit + ybit * (1 - 2 * core)
    y_id = me + 4 - 8 * ybit

    load = pltpu.make_async_copy(emb_hbm, own, load_sem)
    load.start()
    barrier = pltpu.get_barrier_semaphore()
    for other in (mate_id, x_id, y_id):
        pl.semaphore_signal(barrier, inc=1, device_id={"seq": other}, device_id_type=MESH)
    load.wait()
    pl.semaphore_wait(barrier, 3)

    def send(src, dst, send_sem, recv_sem, other):
        copy = pltpu.make_async_remote_copy(
            src_ref=src, dst_ref=dst, send_sem=send_sem, recv_sem=recv_sem,
            device_id={"seq": other}, device_id_type=MESH,
        )
        copy.start()
        return copy

    x_copies, y_copies = [], []
    for k in range(PIECES):
        part = pl.ds(k * piece, piece)
        x_copies.append(send(own.at[part], xblk.at[part], x_send.at[k], x_recv.at[k], x_id))
        y_copies.append(send(own.at[part], yblk.at[part], y_send.at[k], y_recv.at[k], y_id))
    mate_copy = send(own, mate, mate_sems.at[0], mate_sems.at[1], mate_id)

    lowest = jnp.full((1, rows), -1.0, jnp.float32)
    across = jnp.broadcast_to(rank_ref[...].astype(jnp.float32), (rows, rows))
    down = across.T
    self_sims = lax.dot_general(
        own[...], own[...], (((1,), (1,)), ((), ())), preferred_element_type=jnp.float32
    )
    prior = jnp.max(jnp.where(down < across, self_sims, -1.0), axis=0, keepdims=True)
    later = jnp.max(jnp.where(down > across, self_sims, -1.0), axis=0, keepdims=True)

    def fold(prior, later, values, is_prior):
        return (
            jnp.maximum(prior, jnp.where(is_prior, values, lowest)),
            jnp.maximum(later, jnp.where(is_prior, lowest, values)),
        )

    mate_copy.wait_recv()
    prior, later = fold(prior, later, column_max(mate[...], own[...]), core == 1)

    own_x = own_y = mate_x = mate_y = lowest
    x_best = [lowest[:, :piece]] * PIECES
    y_best = [lowest[:, :piece]] * PIECES

    def meet(best, count, left, right):
        found = column_max(left, right)
        return [
            jnp.maximum(b, found[:, j * piece:(j + 1) * piece]) if j < count else b
            for j, b in enumerate(best)
        ]

    for k in range(PIECES):
        x_copies[k].wait_recv()
        y_copies[k].wait_recv()
        start, end = k * piece, (k + 1) * piece
        y_best = meet(y_best, k + 1, xblk[start:end], yblk[:end])
        x_best = meet(x_best, k + 1, yblk[start:end], xblk[:end])
        if k:
            y_best[k] = jnp.maximum(y_best[k], column_max(xblk[:start], yblk[start:end]))
            x_best[k] = jnp.maximum(x_best[k], column_max(yblk[:start], xblk[start:end]))
        if k == PIECES - 1:
            x_out[...] = jnp.concatenate(x_best, axis=1)
            y_out[...] = jnp.concatenate(y_best, axis=1)
            x_back = send(x_out, x_in, back_send.at[0], back_recv.at[0], x_id)
            y_back = send(y_out, y_in, back_send.at[1], back_recv.at[1], y_id)
        mate_x = jnp.maximum(mate_x, column_max(xblk[start:end], mate[...]))
        mate_y = jnp.maximum(mate_y, column_max(yblk[start:end], mate[...]))
        if k == PIECES - 1:
            mate_out[0:1, :] = mate_x
            mate_out[1:2, :] = mate_y
            mate_back = send(mate_out, mate_in, back_send.at[2], back_recv.at[2], mate_id)
        own_x = jnp.maximum(own_x, column_max(xblk[start:end], own[...]))
        own_y = jnp.maximum(own_y, column_max(yblk[start:end], own[...]))

    mate_back.wait_recv()
    chip, x_chip, y_chip = 2 * ybit + xbit, 2 * ybit + 1 - xbit, 2 - 2 * ybit + xbit
    far_chip = 3 - chip
    prior, later = fold(prior, later, jnp.maximum(own_x, mate_in[0:1, :]), x_chip < chip)
    prior, later = fold(prior, later, jnp.maximum(own_y, mate_in[1:2, :]), y_chip < chip)
    x_back.wait_recv()
    y_back.wait_recv()
    prior, later = fold(prior, later, jnp.maximum(x_in[...], y_in[...]), far_chip < chip)
    prior_ref[...] = prior
    later_ref[...] = later
    for copy in [*x_copies, *y_copies, mate_copy, x_back, y_back, mate_back]:
        copy.wait_send()


def exchange(embeddings, doc_order):
    rows, width = embeddings.shape
    block = pltpu.VMEM((rows, width), embeddings.dtype)
    one, two = pltpu.VMEM((1, rows), jnp.float32), pltpu.VMEM((2, rows), jnp.float32)
    dma = pltpu.SemaphoreType.DMA
    result = jax.ShapeDtypeStruct((1, rows), jnp.float32)
    vmem = pl.BlockSpec(memory_space=pltpu.VMEM)
    prior, later = pl.pallas_call(
        exchange_kernel,
        out_shape=(result, result),
        in_specs=[pl.BlockSpec(memory_space=pl.ANY), vmem],
        out_specs=(vmem, vmem),
        scratch_shapes=[
            block, block, block, block, two, one, one, two, one, one,
            dma, dma((2,)), dma((PIECES,)), dma((PIECES,)), dma((PIECES,)), dma((PIECES,)),
            dma((3,)), dma((3,)),
        ],
        compiler_params=pltpu.CompilerParams(collective_id=0, has_side_effects=True),
    )(embeddings, doc_order)
    return prior.reshape(rows), later.reshape(rows)


def passed_along(block, axis, distance):
    devices = range(lax.axis_size(axis))
    route = [((i - distance) % len(devices), i) for i in devices]
    return lax.ppermute(block, axis, route)


def similar(left_rows, right_rows):
    return jnp.einsum("rd,cd->rc", left_rows, right_rows, preferred_element_type=jnp.float32)


def masked_rowmax(matrix, keep):
    return jnp.max(jnp.where(keep, matrix, jnp.float32(-1.0)), axis=1)


def ring_exchange(embeddings, doc_order):
    ranking = doc_order[0]
    position = lax.axis_index("seq")
    members = lax.axis_size("seq")
    block_rows = embeddings.shape[0]
    self_sims = similar(embeddings, embeddings)
    prior_start = masked_rowmax(self_sims, ranking[None, :] < ranking[:, None])
    later_start = masked_rowmax(self_sims, ranking[None, :] > ranking[:, None])
    halfway = members // 2
    table_init = jnp.full((members, 2, block_rows), -1.0, jnp.float32)

    def visit(turn_index, carried):
        visitor, prior_now, later_now, table = carried
        visitor = passed_along(visitor, "seq", 1)
        sims_here = similar(embeddings, visitor)
        row_best = jnp.max(sims_here, axis=1)
        column_best = jnp.max(sims_here, axis=0)
        wrapped = turn_index > position
        active = (turn_index < halfway) | (position >= halfway)
        source = (position - turn_index + members) % members
        prior_now = jnp.where(
            active & jnp.logical_not(wrapped), jnp.maximum(prior_now, row_best), prior_now
        )
        later_now = jnp.where(active & wrapped, jnp.maximum(later_now, row_best), later_now)
        negative = jnp.full((block_rows,), -1.0, jnp.float32)
        entry_prior = jnp.where(active & wrapped, column_best, negative)
        entry_later = jnp.where(active & jnp.logical_not(wrapped), column_best, negative)
        entry = jnp.stack([entry_prior, entry_later], axis=0)[None]
        table = lax.dynamic_update_slice(table, entry, (source, jnp.int32(0), jnp.int32(0)))
        return (visitor, prior_now, later_now, table)

    visitor, prior_now, later_now, table = lax.fori_loop(
        1, halfway + 1, visit, (embeddings, prior_start, later_start, table_init)
    )
    received = lax.all_to_all(table, "seq", split_axis=0, concat_axis=0, tiled=True)
    best_seen = jnp.max(received, axis=0)
    prior_max = jnp.maximum(prior_now, best_seen[0])
    later_max = jnp.maximum(later_now, best_seen[1])
    return (prior_max, later_max)


def per_device(embeddings, doc_order):
    if lax.axis_size("seq") == 2 ** 3:
        return exchange(embeddings, doc_order)
    return ring_exchange(embeddings, doc_order)


def solution(mesh):
    return jax.shard_map(
        per_device,
        mesh=mesh,
        in_specs=(P(("clus", "seq"), None), P(("clus", "seq"), None)),
        out_specs=(P(("clus", "seq")), P(("clus", "seq"))),
        check_vma=False,
    )
```

```python
import functools

import jax
import jax.numpy as jnp
from jax import lax
from jax.experimental import pallas as pl
from jax.experimental.pallas import tpu as pltpu
from jax.sharding import PartitionSpec as P

MESH = pl.DeviceIdType.MESH
PIECES = 2


def column_max(left, right):
    sims = lax.dot_general(
        left, right, (((1,), (1,)), ((), ())), preferred_element_type=jnp.float32
    )
    return jnp.max(sims, axis=0, keepdims=True)


def exchange_kernel(
    emb_hbm, rank_hbm, result_ref,
    rank, own, mate, xblk, yblk, mate_out, x_out, y_out, mate_in, x_in, y_in,
    load_sem, rank_sem, mate_sems, x_send, x_recv, y_send, y_recv, back_send, back_recv,
):
    me = lax.axis_index("seq")
    core, xbit, ybit = me % 2, (me // 2) % 2, me // 4
    rows = own.shape[0]
    piece = rows // PIECES
    mate_id = me + 1 - 2 * core
    x_id = me + 2 - 4 * xbit + ybit * (1 - 2 * core)
    y_id = me + 4 - 8 * ybit

    load = pltpu.make_async_copy(emb_hbm, own, load_sem)
    load.start()
    rank_load = pltpu.make_async_copy(rank_hbm, rank, rank_sem)
    rank_load.start()
    barrier = pltpu.get_barrier_semaphore()
    for other in (mate_id, x_id, y_id):
        pl.semaphore_signal(barrier, inc=1, device_id={"seq": other}, device_id_type=MESH)
    load.wait()
    pl.semaphore_wait(barrier, 3)

    def send(src, dst, send_sem, recv_sem, other):
        copy = pltpu.make_async_remote_copy(
            src_ref=src, dst_ref=dst, send_sem=send_sem, recv_sem=recv_sem,
            device_id={"seq": other}, device_id_type=MESH,
        )
        copy.start()
        return copy

    x_copies, y_copies = [], []
    for k in range(PIECES):
        part = pl.ds(k * piece, piece)
        x_copies.append(send(own.at[part], xblk.at[part], x_send.at[k], x_recv.at[k], x_id))
        y_copies.append(send(own.at[part], yblk.at[part], y_send.at[k], y_recv.at[k], y_id))
    mate_copy = send(own, mate, mate_sems.at[0], mate_sems.at[1], mate_id)

    lowest = jnp.full((1, rows), -1.0, jnp.float32)
    rank_load.wait()
    across = jnp.broadcast_to(rank[...].astype(jnp.float32), (rows, rows))
    down = across.T
    self_sims = lax.dot_general(
        own[...], own[...], (((1,), (1,)), ((), ())), preferred_element_type=jnp.float32
    )
    prior = jnp.max(jnp.where(down < across, self_sims, -1.0), axis=0, keepdims=True)
    later = jnp.max(jnp.where(down > across, self_sims, -1.0), axis=0, keepdims=True)

    def fold(prior, later, values, is_prior):
        return (
            jnp.maximum(prior, jnp.where(is_prior, values, lowest)),
            jnp.maximum(later, jnp.where(is_prior, lowest, values)),
        )

    mate_copy.wait_recv()
    prior, later = fold(prior, later, column_max(mate[...], own[...]), core == 1)

    own_x = own_y = mate_x = mate_y = lowest
    x_best = [lowest[:, :piece]] * PIECES
    y_best = [lowest[:, :piece]] * PIECES

    def meet(best, count, left, right):
        found = column_max(left, right)
        return [
            jnp.maximum(b, found[:, j * piece:(j + 1) * piece]) if j < count else b
            for j, b in enumerate(best)
        ]

    for k in range(PIECES):
        x_copies[k].wait_recv()
        y_copies[k].wait_recv()
        start, end = k * piece, (k + 1) * piece
        y_best = meet(y_best, k + 1, xblk[start:end], yblk[:end])
        x_best = meet(x_best, k + 1, yblk[start:end], xblk[:end])
        if k:
            y_best[k] = jnp.maximum(y_best[k], column_max(xblk[:start], yblk[start:end]))
            x_best[k] = jnp.maximum(x_best[k], column_max(yblk[:start], xblk[start:end]))
        if k == PIECES - 1:
            x_out[...] = jnp.concatenate(x_best, axis=1)
            y_out[...] = jnp.concatenate(y_best, axis=1)
            x_back = send(x_out, x_in, back_send.at[0], back_recv.at[0], x_id)
            y_back = send(y_out, y_in, back_send.at[1], back_recv.at[1], y_id)
        mate_x = jnp.maximum(mate_x, column_max(xblk[start:end], mate[...]))
        mate_y = jnp.maximum(mate_y, column_max(yblk[start:end], mate[...]))
        if k == PIECES - 1:
            mate_out[0:1, :] = mate_x
            mate_out[1:2, :] = mate_y
            mate_back = send(mate_out, mate_in, back_send.at[2], back_recv.at[2], mate_id)
        own_x = jnp.maximum(own_x, column_max(xblk[start:end], own[...]))
        own_y = jnp.maximum(own_y, column_max(yblk[start:end], own[...]))

    mate_back.wait_recv()
    chip, x_chip, y_chip = 2 * ybit + xbit, 2 * ybit + 1 - xbit, 2 - 2 * ybit + xbit
    far_chip = 3 - chip
    prior, later = fold(prior, later, jnp.maximum(own_x, mate_in[0:1, :]), x_chip < chip)
    prior, later = fold(prior, later, jnp.maximum(own_y, mate_in[1:2, :]), y_chip < chip)
    x_back.wait_recv()
    y_back.wait_recv()
    prior, later = fold(prior, later, jnp.maximum(x_in[...], y_in[...]), far_chip < chip)
    result_ref[0:1, :] = prior
    result_ref[1:2, :] = later
    for copy in [*x_copies, *y_copies, mate_copy, x_back, y_back, mate_back]:
        copy.wait_send()


def exchange(embeddings, doc_order):
    rows, width = embeddings.shape
    block = pltpu.VMEM((rows, width), embeddings.dtype)
    one, two = pltpu.VMEM((1, rows), jnp.float32), pltpu.VMEM((2, rows), jnp.float32)
    dma = pltpu.SemaphoreType.DMA
    result = pl.pallas_call(
        exchange_kernel,
        out_shape=two,
        in_specs=[pl.BlockSpec(memory_space=pl.ANY)] * 2,
        out_specs=pl.BlockSpec(memory_space=pltpu.VMEM),
        scratch_shapes=[
            pltpu.VMEM((1, rows), doc_order.dtype), block, block, block, block, two, one, one, two, one, one,
            dma, dma, dma((2,)), dma((PIECES,)), dma((PIECES,)), dma((PIECES,)), dma((PIECES,)),
            dma((3,)), dma((3,)),
        ],
        compiler_params=pltpu.CompilerParams(collective_id=0, has_side_effects=True),
    )(embeddings, doc_order)
    return result[0], result[1]


def passed_along(block, axis, distance):
    devices = range(lax.axis_size(axis))
    route = [((i - distance) % len(devices), i) for i in devices]
    return lax.ppermute(block, axis, route)


def similar(left_rows, right_rows):
    return jnp.einsum("rd,cd->rc", left_rows, right_rows, preferred_element_type=jnp.float32)


def masked_rowmax(matrix, keep):
    return jnp.max(jnp.where(keep, matrix, jnp.float32(-1.0)), axis=1)


def ring_exchange(embeddings, doc_order):
    ranking = doc_order[0]
    position = lax.axis_index("seq")
    members = lax.axis_size("seq")
    block_rows = embeddings.shape[0]
    self_sims = similar(embeddings, embeddings)
    prior_start = masked_rowmax(self_sims, ranking[None, :] < ranking[:, None])
    later_start = masked_rowmax(self_sims, ranking[None, :] > ranking[:, None])
    halfway = members // 2
    table_init = jnp.full((members, 2, block_rows), -1.0, jnp.float32)

    def visit(turn_index, carried):
        visitor, prior_now, later_now, table = carried
        visitor = passed_along(visitor, "seq", 1)
        sims_here = similar(embeddings, visitor)
        row_best = jnp.max(sims_here, axis=1)
        column_best = jnp.max(sims_here, axis=0)
        wrapped = turn_index > position
        active = (turn_index < halfway) | (position >= halfway)
        source = (position - turn_index + members) % members
        prior_now = jnp.where(
            active & jnp.logical_not(wrapped), jnp.maximum(prior_now, row_best), prior_now
        )
        later_now = jnp.where(active & wrapped, jnp.maximum(later_now, row_best), later_now)
        negative = jnp.full((block_rows,), -1.0, jnp.float32)
        entry_prior = jnp.where(active & wrapped, column_best, negative)
        entry_later = jnp.where(active & jnp.logical_not(wrapped), column_best, negative)
        entry = jnp.stack([entry_prior, entry_later], axis=0)[None]
        table = lax.dynamic_update_slice(table, entry, (source, jnp.int32(0), jnp.int32(0)))
        return (visitor, prior_now, later_now, table)

    visitor, prior_now, later_now, table = lax.fori_loop(
        1, halfway + 1, visit, (embeddings, prior_start, later_start, table_init)
    )
    received = lax.all_to_all(table, "seq", split_axis=0, concat_axis=0, tiled=True)
    best_seen = jnp.max(received, axis=0)
    prior_max = jnp.maximum(prior_now, best_seen[0])
    later_max = jnp.maximum(later_now, best_seen[1])
    return (prior_max, later_max)


def per_device(embeddings, doc_order):
    if lax.axis_size("seq") == 2 ** 3:
        return exchange(embeddings, doc_order)
    return ring_exchange(embeddings, doc_order)


def solution(mesh):
    return jax.shard_map(
        per_device,
        mesh=mesh,
        in_specs=(P(("clus", "seq"), None), P(("clus", "seq"), None)),
        out_specs=(P(("clus", "seq")), P(("clus", "seq"))),
        check_vma=False,
    )
```

```python
import functools

import jax
import jax.numpy as jnp
from jax import lax
from jax.experimental import pallas as pl
from jax.experimental.pallas import tpu as pltpu
from jax.sharding import PartitionSpec as P

MESH = pl.DeviceIdType.MESH
PIECES = 1


def column_max(left, right):
    sims = lax.dot_general(
        left, right, (((1,), (1,)), ((), ())), preferred_element_type=jnp.float32
    )
    return jnp.max(sims, axis=0, keepdims=True)


def exchange_kernel(
    emb_hbm, rank_hbm, result_ref,
    rank, own, mate, xblk, yblk, mate_out, x_out, y_out, mate_in, x_in, y_in,
    load_sem, rank_sem, mate_sems, x_send, x_recv, y_send, y_recv, back_send, back_recv,
):
    me = lax.axis_index("seq")
    core, xbit, ybit = me % 2, (me // 2) % 2, me // 4
    rows = own.shape[0]
    piece = rows // PIECES
    mate_id = me + 1 - 2 * core
    x_id = me + 2 - 4 * xbit + (1 - 2 * core)
    y_id = me + 4 - 8 * ybit + (1 - xbit) * (1 - 2 * core)

    barrier = pltpu.get_barrier_semaphore()
    for other in (x_id, y_id, mate_id):
        pl.semaphore_signal(barrier, inc=1, device_id={"seq": other}, device_id_type=MESH)
    load = pltpu.make_async_copy(emb_hbm, own, load_sem)
    load.start()
    rank_load = pltpu.make_async_copy(rank_hbm, rank, rank_sem)
    rank_load.start()
    load.wait()
    pl.semaphore_wait(barrier, 3)

    def send(src, dst, send_sem, recv_sem, other):
        copy = pltpu.make_async_remote_copy(
            src_ref=src, dst_ref=dst, send_sem=send_sem, recv_sem=recv_sem,
            device_id={"seq": other}, device_id_type=MESH,
        )
        copy.start()
        return copy

    x_copies, y_copies = [], []
    for k in range(PIECES):
        part = pl.ds(k * piece, piece)
        x_copies.append(send(own.at[part], xblk.at[part], x_send.at[k], x_recv.at[k], x_id))
        y_copies.append(send(own.at[part], yblk.at[part], y_send.at[k], y_recv.at[k], y_id))
    mate_copy = send(own, mate, mate_sems.at[0], mate_sems.at[1], mate_id)

    lowest = jnp.full((1, rows), -1.0, jnp.float32)
    rank_load.wait()
    across = jnp.broadcast_to(rank[...].astype(jnp.float32), (rows, rows))
    down = across.T
    self_sims = lax.dot_general(
        own[...], own[...], (((1,), (1,)), ((), ())), preferred_element_type=jnp.float32
    )
    prior = jnp.max(jnp.where(down < across, self_sims, -1.0), axis=0, keepdims=True)
    later = jnp.max(jnp.where(down > across, self_sims, -1.0), axis=0, keepdims=True)

    def fold(prior, later, values, is_prior):
        return (
            jnp.maximum(prior, jnp.where(is_prior, values, lowest)),
            jnp.maximum(later, jnp.where(is_prior, lowest, values)),
        )

    mate_copy.wait_recv()
    prior, later = fold(prior, later, column_max(mate[...], own[...]), core == 1)

    own_x = own_y = mate_x = mate_y = lowest
    x_best = [lowest[:, :piece]] * PIECES
    y_best = [lowest[:, :piece]] * PIECES

    def meet(best, count, left, right):
        found = column_max(left, right)
        return [
            jnp.maximum(b, found[:, j * piece:(j + 1) * piece]) if j < count else b
            for j, b in enumerate(best)
        ]

    for k in range(PIECES):
        x_copies[k].wait_recv()
        y_copies[k].wait_recv()
        start, end = k * piece, (k + 1) * piece
        y_best = meet(y_best, k + 1, xblk[start:end], yblk[:end])
        x_best = meet(x_best, k + 1, yblk[start:end], xblk[:end])
        if k:
            y_best[k] = jnp.maximum(y_best[k], column_max(xblk[:start], yblk[start:end]))
            x_best[k] = jnp.maximum(x_best[k], column_max(yblk[:start], xblk[start:end]))
        if k == PIECES - 1:
            x_out[...] = jnp.concatenate(x_best, axis=1)
            y_out[...] = jnp.concatenate(y_best, axis=1)
            x_back = send(x_out, x_in, back_send.at[0], back_recv.at[0], x_id)
            y_back = send(y_out, y_in, back_send.at[1], back_recv.at[1], y_id)
        mate_x = jnp.maximum(mate_x, column_max(xblk[start:end], mate[...]))
        mate_y = jnp.maximum(mate_y, column_max(yblk[start:end], mate[...]))
        if k == PIECES - 1:
            mate_out[0:1, :] = mate_x
            mate_out[1:2, :] = mate_y
            mate_back = send(mate_out, mate_in, back_send.at[2], back_recv.at[2], mate_id)
        own_x = jnp.maximum(own_x, column_max(xblk[start:end], own[...]))
        own_y = jnp.maximum(own_y, column_max(yblk[start:end], own[...]))

    mate_back.wait_recv()
    chip, x_chip, y_chip = 2 * ybit + xbit, 2 * ybit + 1 - xbit, 2 - 2 * ybit + xbit
    far_chip = 3 - chip
    prior, later = fold(prior, later, jnp.maximum(own_x, mate_in[0:1, :]), x_chip < chip)
    prior, later = fold(prior, later, jnp.maximum(own_y, mate_in[1:2, :]), y_chip < chip)
    x_back.wait_recv()
    y_back.wait_recv()
    prior, later = fold(prior, later, jnp.maximum(x_in[...], y_in[...]), far_chip < chip)
    result_ref[0:1, :] = prior
    result_ref[1:2, :] = later
    for copy in [*x_copies, *y_copies, mate_copy, x_back, y_back, mate_back]:
        copy.wait_send()


def exchange(embeddings, doc_order):
    rows, width = embeddings.shape
    block = pltpu.VMEM((rows, width), embeddings.dtype)
    one, two = pltpu.VMEM((1, rows), jnp.float32), pltpu.VMEM((2, rows), jnp.float32)
    dma = pltpu.SemaphoreType.DMA
    result = pl.pallas_call(
        exchange_kernel,
        out_shape=two,
        in_specs=[pl.BlockSpec(memory_space=pl.ANY)] * 2,
        out_specs=pl.BlockSpec(memory_space=pltpu.VMEM),
        scratch_shapes=[
            pltpu.VMEM((1, rows), doc_order.dtype), block, block, block, block, two, one, one, two, one, one,
            dma, dma, dma((2,)), dma((PIECES,)), dma((PIECES,)), dma((PIECES,)), dma((PIECES,)),
            dma((3,)), dma((3,)),
        ],
        compiler_params=pltpu.CompilerParams(collective_id=0, has_side_effects=True),
    )(embeddings, doc_order)
    return result[0], result[1]


def passed_along(block, axis, distance):
    devices = range(lax.axis_size(axis))
    route = [((i - distance) % len(devices), i) for i in devices]
    return lax.ppermute(block, axis, route)


def similar(left_rows, right_rows):
    return jnp.einsum("rd,cd->rc", left_rows, right_rows, preferred_element_type=jnp.float32)


def masked_rowmax(matrix, keep):
    return jnp.max(jnp.where(keep, matrix, jnp.float32(-1.0)), axis=1)


def ring_exchange(embeddings, doc_order):
    ranking = doc_order[0]
    position = lax.axis_index("seq")
    members = lax.axis_size("seq")
    block_rows = embeddings.shape[0]
    self_sims = similar(embeddings, embeddings)
    prior_start = masked_rowmax(self_sims, ranking[None, :] < ranking[:, None])
    later_start = masked_rowmax(self_sims, ranking[None, :] > ranking[:, None])
    halfway = members // 2
    table_init = jnp.full((members, 2, block_rows), -1.0, jnp.float32)

    def visit(turn_index, carried):
        visitor, prior_now, later_now, table = carried
        visitor = passed_along(visitor, "seq", 1)
        sims_here = similar(embeddings, visitor)
        row_best = jnp.max(sims_here, axis=1)
        column_best = jnp.max(sims_here, axis=0)
        wrapped = turn_index > position
        active = (turn_index < halfway) | (position >= halfway)
        source = (position - turn_index + members) % members
        prior_now = jnp.where(
            active & jnp.logical_not(wrapped), jnp.maximum(prior_now, row_best), prior_now
        )
        later_now = jnp.where(active & wrapped, jnp.maximum(later_now, row_best), later_now)
        negative = jnp.full((block_rows,), -1.0, jnp.float32)
        entry_prior = jnp.where(active & wrapped, column_best, negative)
        entry_later = jnp.where(active & jnp.logical_not(wrapped), column_best, negative)
        entry = jnp.stack([entry_prior, entry_later], axis=0)[None]
        table = lax.dynamic_update_slice(table, entry, (source, jnp.int32(0), jnp.int32(0)))
        return (visitor, prior_now, later_now, table)

    visitor, prior_now, later_now, table = lax.fori_loop(
        1, halfway + 1, visit, (embeddings, prior_start, later_start, table_init)
    )
    received = lax.all_to_all(table, "seq", split_axis=0, concat_axis=0, tiled=True)
    best_seen = jnp.max(received, axis=0)
    prior_max = jnp.maximum(prior_now, best_seen[0])
    later_max = jnp.maximum(later_now, best_seen[1])
    return (prior_max, later_max)


def per_device(embeddings, doc_order):
    if lax.axis_size("seq") == 2 ** 3:
        return exchange(embeddings, doc_order)
    return ring_exchange(embeddings, doc_order)


def solution(mesh):
    return jax.shard_map(
        per_device,
        mesh=mesh,
        in_specs=(P(("clus", "seq"), None), P(("clus", "seq"), None)),
        out_specs=(P(("clus", "seq")), P(("clus", "seq"))),
        check_vma=False,
    )
```
